32 devices in a mesh: heads: 8 (over z, y), model: 4 (over x, core).
Axes of the slice: x: 2, y: 2, z: 4, core: 2. Of those that a mesh axis runs over, the one named last changes fastest.
Arguments:
- hidden_in: bfloat16 [2048, 3840], P(None, 'model')
- seg_ids: int32 [2048], replicated
- positions: int32 [2048], replicated
- w_query: bfloat16 [2, 3840, 4096], P(None, 'model', 'heads')
- w_key: bfloat16 [2, 3840, 2048], P(None, 'model', 'heads')
- w_value: bfloat16 [2, 3840, 2048], P(None, 'model', 'heads')
- w_out: bfloat16 [2, 4096, 3840], P(None, 'heads', 'model')
- w_gate: bfloat16 [2, 3840, 15360], P(None, 'model', 'heads')
- w_up: bfloat16 [2, 3840, 15360], P(None, 'model', 'heads')
- w_down: bfloat16 [2, 15360, 3840], P(None, 'heads', 'model')
- norm_scales: float32 [2, 4, 3840], P(None, None, 'model')
- qk_scales: float32 [2, 2, 256], replicated
Outputs:
- output 1: bfloat16 [2048, 3840], P(None, 'model')
- output 2: bfloat16 [2, 2048, 8, 256], P(None, None, 'heads')
- output 3: bfloat16 [2, 2048, 8, 256], P(None, None, 'heads')
All inputs are finite; a program needn't handle non-finite values.
Results may differ from the reference program's by a relative error of at most 0.02.
Values are sent between devices in bfloat16 or wider.
A program may use at most 1 GiB of HBM per device.

```python
import jax
import jax.numpy as jnp
from jax import lax

TOKENS = 2048
D_MODEL = 3840
Q_HEADS = 16
KV_HEADS = 8
HEAD_DIM = 256
FFN_DIM = 15360
WINDOW = 1024
REQUESTS = 8
Q_BLOCK = 256
OUTLIERS = 8
NORM_EPS = 1e-6
GLOBAL_BASE = 1000000.0
GLOBAL_FACTOR = 8.0
LOCAL_BASE = 10000.0


def draw_requests(rng_key):
    cut_points = jnp.sort(jax.random.permutation(rng_key, TOKENS - 1)[:REQUESTS - 1] + 1).astype(jnp.int32)
    tok_index = jnp.arange(TOKENS, dtype=jnp.int32)
    seg_ids = jnp.sum((tok_index[:, None] >= cut_points[None, :]).astype(jnp.int32), axis=1)
    starts = jnp.concatenate([jnp.zeros((1,), jnp.int32), cut_points])
    positions = tok_index - starts[seg_ids]
    return seg_ids.astype(jnp.int32), positions.astype(jnp.int32)


def gauss_weight(rng_key, arr_shape, fan_in):
    return jax.random.normal(rng_key, arr_shape, jnp.float32) * (fan_in ** -0.5)


def setup_inputs(seed: int = 0) -> dict:
    rng_keys = jax.random.split(jax.random.key(seed), 16)
    seg_ids, positions = draw_requests(rng_keys[0])
    col_scale = jnp.exp(0.6 * jax.random.normal(rng_keys[1], (D_MODEL,), jnp.float32))
    hot_cols = jax.random.permutation(rng_keys[2], D_MODEL)[:OUTLIERS]
    col_scale = col_scale.at[hot_cols].set(20.0)
    hidden = jax.random.normal(rng_keys[3], (TOKENS, D_MODEL), jnp.float32) * col_scale[None, :]
    hidden = hidden * lax.rsqrt(jnp.mean(hidden * hidden))
    q_width = Q_HEADS * HEAD_DIM
    kv_width = KV_HEADS * HEAD_DIM
    out_cols = jnp.exp(0.5 * jax.random.normal(rng_keys[4], (2, 1, D_MODEL), jnp.float32))
    down_cols = jnp.exp(0.5 * jax.random.normal(rng_keys[5], (2, 1, D_MODEL), jnp.float32))
    return {
        'hidden_in': hidden.astype(jnp.bfloat16),
        'seg_ids': seg_ids,
        'positions': positions,
        'w_query': gauss_weight(rng_keys[6], (2, D_MODEL, q_width), D_MODEL).astype(jnp.bfloat16),
        'w_key': gauss_weight(rng_keys[7], (2, D_MODEL, kv_width), D_MODEL).astype(jnp.bfloat16),
        'w_value': gauss_weight(rng_keys[8], (2, D_MODEL, kv_width), D_MODEL).astype(jnp.bfloat16),
        'w_out': (gauss_weight(rng_keys[9], (2, q_width, D_MODEL), q_width) * out_cols).astype(jnp.bfloat16),
        'w_gate': gauss_weight(rng_keys[10], (2, D_MODEL, FFN_DIM), D_MODEL).astype(jnp.bfloat16),
        'w_up': gauss_weight(rng_keys[11], (2, D_MODEL, FFN_DIM), D_MODEL).astype(jnp.bfloat16),
        'w_down': (gauss_weight(rng_keys[12], (2, FFN_DIM, D_MODEL), FFN_DIM) * down_cols).astype(jnp.bfloat16),
        'norm_scales': 0.5 * jax.random.normal(rng_keys[13], (2, 4, D_MODEL), jnp.float32),
        'qk_scales': 0.5 * jax.random.normal(rng_keys[14], (2, 2, HEAD_DIM), jnp.float32),
    }


def gemma_norm(values, scale_row):
    mean_sq = jnp.mean(values * values, axis=-1, keepdims=True)
    return values * lax.rsqrt(mean_sq + NORM_EPS) * (1.0 + scale_row)


def rope_tables(positions, rope_base, pos_factor):
    exponents = jnp.arange(0, HEAD_DIM, 2).astype(jnp.float32) / HEAD_DIM
    inv_freq = rope_base ** (-exponents)
    angles = (positions.astype(jnp.float32) / pos_factor)[:, None] * inv_freq[None, :]
    return jnp.cos(angles), jnp.sin(angles)


def apply_rope(values, cos_tab, sin_tab):
    half_dim = values.shape[-1] // 2
    first_half = values[..., :half_dim]
    second_half = values[..., half_dim:]
    cos_bcast = cos_tab[:, None, :]
    sin_bcast = sin_tab[:, None, :]
    return jnp.concatenate([first_half * cos_bcast - second_half * sin_bcast, second_half * cos_bcast + first_half * sin_bcast], axis=-1)


def attend(query_heads, key_heads, value_heads, seg_ids, positions, window):
    group_size = Q_HEADS // KV_HEADS
    n_blocks = TOKENS // Q_BLOCK
    q_scale = HEAD_DIM ** -0.5
    key_f32 = key_heads.astype(jnp.float32)
    value_f32 = value_heads.astype(jnp.float32)
    q_blocks = query_heads.reshape(n_blocks, Q_BLOCK, KV_HEADS, group_size, HEAD_DIM)
    seg_blocks = seg_ids.reshape(n_blocks, Q_BLOCK)
    pos_blocks = positions.reshape(n_blocks, Q_BLOCK)

    def one_block(block_args):
        q_blk, seg_blk, pos_blk = block_args
        scores = jnp.einsum('qkgd,tkd->kgqt', q_blk.astype(jnp.float32), key_f32) * q_scale
        pos_gap = pos_blk[:, None] - positions[None, :]
        allowed = (seg_blk[:, None] == seg_ids[None, :]) & (pos_gap >= 0) & (pos_gap < window)
        scores = jnp.where(allowed[None, None], scores, -1e30)
        row_max = jnp.max(scores, axis=-1, keepdims=True)
        exp_scores = jnp.exp(scores - row_max)
        probs_bf = (exp_scores / jnp.sum(exp_scores, axis=-1, keepdims=True)).astype(jnp.bfloat16)
        blk_out = jnp.einsum('kgqt,tkd->qkgd', probs_bf.astype(jnp.float32), value_f32)
        return blk_out.astype(jnp.bfloat16)

    attn_out = lax.map(one_block, (q_blocks, seg_blocks, pos_blocks))
    return attn_out.reshape(TOKENS, Q_HEADS * HEAD_DIM)


def run_layer(hidden, seg_ids, positions, layer_w, norm_row, qk_row, rope_base, pos_factor, window):
    w_query, w_key, w_value, w_out, w_gate, w_up, w_down = layer_w
    resid_f32 = hidden.astype(jnp.float32)
    normed = gemma_norm(resid_f32, norm_row[0]).astype(jnp.bfloat16)
    query_bf = jnp.dot(normed, w_query, preferred_element_type=jnp.float32).astype(jnp.bfloat16)
    keys_bf = jnp.dot(normed, w_key, preferred_element_type=jnp.float32).astype(jnp.bfloat16)
    values_bf = jnp.dot(normed, w_value, preferred_element_type=jnp.float32).astype(jnp.bfloat16)
    cos_tab, sin_tab = rope_tables(positions, rope_base, pos_factor)
    query_heads = apply_rope(gemma_norm(query_bf.astype(jnp.float32).reshape(TOKENS, Q_HEADS, HEAD_DIM), qk_row[0]), cos_tab, sin_tab).astype(jnp.bfloat16)
    key_heads = apply_rope(gemma_norm(keys_bf.astype(jnp.float32).reshape(TOKENS, KV_HEADS, HEAD_DIM), qk_row[1]), cos_tab, sin_tab).astype(jnp.bfloat16)
    value_heads = values_bf.reshape(TOKENS, KV_HEADS, HEAD_DIM)
    attn_out = attend(query_heads, key_heads, value_heads, seg_ids, positions, window)
    attn_sum = jnp.dot(attn_out, w_out, preferred_element_type=jnp.float32).astype(jnp.bfloat16)
    hidden_mid = (resid_f32 + gemma_norm(attn_sum.astype(jnp.float32), norm_row[1])).astype(jnp.bfloat16)
    mid_f32 = hidden_mid.astype(jnp.float32)
    normed_ffn = gemma_norm(mid_f32, norm_row[2]).astype(jnp.bfloat16)
    gate_bf = jnp.dot(normed_ffn, w_gate, preferred_element_type=jnp.float32).astype(jnp.bfloat16)
    up_bf = jnp.dot(normed_ffn, w_up, preferred_element_type=jnp.float32).astype(jnp.bfloat16)
    ffn_in = (jax.nn.gelu(gate_bf.astype(jnp.float32), approximate=True) * up_bf.astype(jnp.float32)).astype(jnp.bfloat16)
    ffn_sum = jnp.dot(ffn_in, w_down, preferred_element_type=jnp.float32).astype(jnp.bfloat16)
    hidden_new = (mid_f32 + gemma_norm(ffn_sum.astype(jnp.float32), norm_row[3])).astype(jnp.bfloat16)
    return hidden_new, key_heads, value_heads


def reference(hidden_in, seg_ids, positions, w_query, w_key, w_value, w_out, w_gate, w_up, w_down, norm_scales, qk_scales):
    settings = ((GLOBAL_BASE, GLOBAL_FACTOR, TOKENS), (LOCAL_BASE, 1.0, WINDOW))
    hidden = hidden_in
    key_list = []
    value_list = []
    for layer_idx in range(2):
        rope_base, pos_factor, window = settings[layer_idx]
        layer_w = (w_query[layer_idx], w_key[layer_idx], w_value[layer_idx], w_out[layer_idx], w_gate[layer_idx], w_up[layer_idx], w_down[layer_idx])
        hidden, key_heads, value_heads = run_layer(hidden, seg_ids, positions, layer_w, norm_scales[layer_idx], qk_scales[layer_idx], rope_base, pos_factor, window)
        key_list.append(key_heads)
        value_list.append(value_heads)
    return hidden, jnp.stack(key_list), jnp.stack(value_list)
```

```python
import functools

import jax
import jax.numpy as jnp
from jax import lax
from jax.experimental import pallas as pl
from jax.experimental.pallas import tpu as pltpu
from jax.sharding import PartitionSpec as P

NORM_EPS = 1e-6
WINDOW = 1024
GLOBAL_BASE = 1000000.0
GLOBAL_FACTOR = 8.0
LOCAL_BASE = 10000.0
MESH = pl.DeviceIdType.MESH
N_ROWS = 64
PIECES = 8
HALF = 32


def remote(src, dst, send_sem, recv_sem, device):
    return pltpu.make_async_remote_copy(src_ref=src, dst_ref=dst, send_sem=send_sem, recv_sem=recv_sem,
                                        device_id=device, device_id_type=MESH)


def move_kernel(mode, *refs):
    if mode == 'first':
        (hid_ref, scale_b_ref, x_out, g_out,
         loc_sem, a2a_s, a2a_r, gr_s, gr_r, gl_s, gl_r, gy_s, gy_r) = refs
    elif mode == 'mid':
        (part_ref, x_ref, scale_a_ref, scale_b_ref, x_out, g_out,
         sums, y_buf, r_buf, l_buf, loc_sem, y_s, y_r, r_s, r_r, l_s, l_r,
         gr_s, gr_r, gl_s, gl_r, gy_s, gy_r) = refs
    else:
        (part_ref, x_ref, scale_a_ref, g_out,
         sums, y_buf, r_buf, l_buf, fin, loc_sem, y_s, y_r, r_s, r_r, l_s, l_r,
         a2a_s, a2a_r, gr_s, gr_r, gl_s, gl_r, gy_s, gy_r) = refs
    head = lax.axis_index('heads')
    m = lax.axis_index('model')
    z = lax.div(head, 2)
    y = lax.rem(head, 2)
    x = lax.div(m, 2)
    c = lax.rem(m, 2)
    flips = [None, x * 2 + (1 - c), (1 - x) * 2 + c, (1 - x) * 2 + (1 - c)]
    y_peer = (z * 2 + 1 - y, m)
    up = (z * 2 + 2 + y, m)
    down = (z * 2 - 2 + y, m)

    barrier = pltpu.get_barrier_semaphore()

    def greet(device):
        pl.semaphore_signal(barrier, inc=1, device_id=device, device_id_type=MESH)

    greet(y_peer)
    pl.when(z < 3)(lambda: greet(up))
    pl.when(z > 0)(lambda: greet(down))
    n_wait = 2
    if mode != 'mid':
        for j in (1, 2, 3):
            greet((head, flips[j]))
        n_wait = 5
    inside = lax.rem(lax.div(z + 1, 2), 2)
    pl.semaphore_wait(barrier, n_wait + inside)

    if mode == 'first':
        own = pltpu.make_async_copy(hid_ref.at[m, head], x_out.at[0], loc_sem.at[0])
        own.start()
        sends = [remote(hid_ref.at[flips[j], head], x_out.at[j], a2a_s.at[j], a2a_r.at[j], (head, flips[j]))
                 for j in (1, 2, 3)]
        for copy in sends:
            copy.start()
        own.wait()
        for copy in sends:
            copy.wait()
    else:
        def at_piece(p):
            return lax.div(p, 2), pl.ds(pl.multiple_of(lax.rem(p, 2) * HALF, HALF), HALF)

        def load_of(p):
            j, rows = at_piece(p)
            return pltpu.make_async_copy(part_ref.at[j, :, y, rows, :], sums.at[j, :, rows, :], loc_sem.at[p])

        def y_of(p):
            j, rows = at_piece(p)
            return remote(part_ref.at[j, :, 1 - y, rows, :], y_buf.at[j, :, rows, :], y_s.at[p], y_r.at[p], y_peer)

        def r_of(t, p):
            j, rows = at_piece(p)
            return remote(sums.at[j, t, rows, :], r_buf.at[t - 1, j, rows, :], r_s.at[t - 1, p], r_r.at[t - 1, p], up)

        def l_of(t, p):
            j, rows = at_piece(p)
            return remote(sums.at[j, t, rows, :], l_buf.at[t, j, rows, :], l_s.at[t, p], l_r.at[t, p], down)

        for p in range(PIECES):
            y_of(p).start()
            load_of(p).start()

        def step(s, carry):
            @pl.when(s < PIECES)
            def _():
                load_of(s).wait()
                y_of(s).wait_recv()
                j, rows = at_piece(s)
                sums[j, :, rows, :] += y_buf[j, :, rows, :]

            p_r = s - z

            @pl.when((p_r >= 0) & (p_r < PIECES))
            def _():
                j, rows = at_piece(p_r)
                for t in (3, 2, 1):
                    @pl.when((z > 0) & (z <= t))
                    def _():
                        r_of(t, p_r).wait_recv()
                        sums[j, t, rows, :] += r_buf[t - 1, j, rows, :]

                    @pl.when(z < t)
                    def _():
                        r_of(t, p_r).start()

            p_l = s - (3 - z)

            @pl.when((p_l >= 0) & (p_l < PIECES))
            def _():
                j, rows = at_piece(p_l)
                for t in (0, 1, 2):
                    @pl.when((z < 3) & (z >= t))
                    def _():
                        l_of(t, p_l).wait_recv()
                        sums[j, t, rows, :] += l_buf[t, j, rows, :]

                    @pl.when(z > t)
                    def _():
                        l_of(t, p_l).start()
            return carry

        lax.fori_loop(0, PIECES + 3, step, 0)

    width = 4 * 960

    def inv_rms(parts):
        total = functools.reduce(lambda a, b: a + b, [jnp.sum(v * v, axis=-1, keepdims=True) for v in parts])
        return lax.rsqrt(total / width + NORM_EPS)

    if mode == 'first':
        rows_new = [x_out[j].astype(jnp.float32) for j in range(4)]
    else:
        added = [sums[j, z].astype(jnp.bfloat16).astype(jnp.float32) for j in range(4)]
        inv = inv_rms(added)
        rows_new = []
        for j in range(4):
            new = (x_ref[j].astype(jnp.float32) + added[j] * inv * (1.0 + scale_a_ref[j])).astype(jnp.bfloat16)
            if mode == 'mid':
                x_out[j] = new
                rows_new.append(new.astype(jnp.float32))
            else:
                fin[j] = new
    if mode != 'last':
        inv = inv_rms(rows_new)
        for j in range(4):
            g_out[j, head] = (rows_new[j] * inv * (1.0 + scale_b_ref[j])).astype(jnp.bfloat16)
    else:
        own = pltpu.make_async_copy(fin.at[0], g_out.at[m, head], loc_sem.at[PIECES])
        own.start()
        sends = [remote(fin.at[j], g_out.at[m, head], a2a_s.at[j], a2a_r.at[j], (head, flips[j])) for j in (1, 2, 3)]
        for copy in sends:
            copy.start()
        own.wait()
        for j, copy in zip((1, 2, 3), sends):
            copy.wait_send()
            remote(fin.at[j], g_out.at[flips[j], head], a2a_s.at[j], a2a_r.at[j], (head, flips[j])).wait_recv()

    def gather(kind, bz):
        send_sems, recv_sems, device = {'r': (gr_s, gr_r, up), 'l': (gl_s, gl_r, down), 'y': (gy_s, gy_r, y_peer)}[kind]
        block = g_out.at[:, bz * 2 + y]
        return remote(block, block, send_sems.at[bz], recv_sems.at[bz], device)

    gather('y', z).start()
    pl.when(z < 3)(lambda: gather('r', z).start())
    pl.when(z > 0)(lambda: gather('l', z).start())
    for d in (1, 2, 3):
        @pl.when(z >= d)
        def _():
            gather('r', z - d).wait_recv()
            pl.when(z < 3)(lambda: gather('r', z - d).start())
            gather('y', z - d).start()

        @pl.when(z + d <= 3)
        def _():
            gather('l', z + d).wait_recv()
            pl.when(z > 0)(lambda: gather('l', z + d).start())
            gather('y', z + d).start()
    for bz in range(4):
        gather('y', bz).wait_send()
        block = g_out.at[:, bz * 2 + 1 - y]
        remote(block, block, gy_s.at[bz], gy_r.at[bz], y_peer).wait_recv()
        pl.when((bz <= z) & (z < 3))(lambda: gather('r', bz).wait_send())
        pl.when((bz >= z) & (z > 0))(lambda: gather('l', bz).wait_send())

    if mode != 'first':
        def drain(p, carry):
            y_of(p).wait_send()
            for t in (1, 2, 3):
                pl.when(z < t)(lambda: r_of(t, p).wait_send())
            for t in (0, 1, 2):
                pl.when(z > t)(lambda: l_of(t, p).wait_send())
            return carry

        lax.fori_loop(0, PIECES, drain, 0)


def move(mode, call_id, *args):
    vmem = pl.BlockSpec(memory_space=pltpu.VMEM)
    hbm = pl.BlockSpec(memory_space=pl.ANY)
    dma = pltpu.SemaphoreType.DMA
    rows_shape = jax.ShapeDtypeStruct((4, N_ROWS, 960), jnp.bfloat16)
    g_shape = jax.ShapeDtypeStruct((4, 8, N_ROWS, 960), jnp.bfloat16)
    ring = [dma((4,))] * 6
    a2a = [dma((4,)), dma((4,))]
    reduce_bufs = [pltpu.VMEM((4, 4, N_ROWS, 960), jnp.float32), pltpu.VMEM((4, 4, N_ROWS, 960), jnp.float32),
                   pltpu.VMEM((3, 4, N_ROWS, 960), jnp.float32), pltpu.VMEM((3, 4, N_ROWS, 960), jnp.float32)]
    reduce_sems = [dma((PIECES + 1,)), dma((PIECES,)), dma((PIECES,))] + [dma((3, PIECES))] * 4
    if mode == 'first':
        in_specs, outs = [hbm, vmem], (rows_shape, g_shape)
        scratch = [dma((1,))] + a2a + ring
    elif mode == 'mid':
        in_specs, outs = [hbm, vmem, vmem, vmem], (rows_shape, g_shape)
        scratch = reduce_bufs + reduce_sems + ring
    else:
        in_specs, outs = [hbm, vmem, vmem], (g_shape,)
        scratch = reduce_bufs + [pltpu.VMEM((4, N_ROWS, 960), jnp.bfloat16)] + reduce_sems + a2a + ring
    micros = {'first': 55, 'mid': 140, 'last': 150}[mode]
    return pl.pallas_call(
        functools.partial(move_kernel, mode),
        out_shape=outs,
        in_specs=in_specs,
        out_specs=tuple(vmem for _ in outs),
        scratch_shapes=scratch,
        name='move_' + mode + str(call_id),
        cost_estimate=pl.CostEstimate(flops=micros * 15_000_000, bytes_accessed=1 << 24, transcendentals=0),
        compiler_params=pltpu.CompilerParams(collective_id=call_id, has_side_effects=True, vmem_limit_bytes=50 << 20),
    )(*args)


def kv_kernel(kv_ref, out_ref, loc_sem, send_sems, recv_sems):
    head = lax.axis_index('heads')
    m = lax.axis_index('model')
    x = lax.div(m, 2)
    c = lax.rem(m, 2)
    m_core, m_x, m_both = x * 2 + 1 - c, (1 - x) * 2 + c, (1 - x) * 2 + 1 - c
    barrier = pltpu.get_barrier_semaphore()
    for peer in (m_core, m_x):
        pl.semaphore_signal(barrier, inc=1, device_id=(head, peer), device_id_type=MESH)
    pl.semaphore_wait(barrier, 2)
    own = pltpu.make_async_copy(kv_ref, out_ref.at[m], loc_sem.at[0])

    def send(slot, src, place, peer):
        return remote(src, out_ref.at[place], send_sems.at[slot], recv_sems.at[slot], (head, peer))

    to_x = send(0, kv_ref, m, m_x)
    to_core = send(1, kv_ref, m, m_core)
    to_x.start()
    to_core.start()
    own.start()
    send(0, kv_ref, m_x, m_x).wait_recv()
    on = send(2, out_ref.at[m_x], m_x, m_core)
    on.start()
    own.wait()
    send(1, kv_ref, m_core, m_core).wait_recv()
    send(2, kv_ref, m_both, m_core).wait_recv()
    to_x.wait_send()
    to_core.wait_send()
    on.wait_send()


def share_kv(call_id, kv):
    vmem = pl.BlockSpec(memory_space=pltpu.VMEM)
    dma = pltpu.SemaphoreType.DMA
    return pl.pallas_call(
        kv_kernel,
        out_shape=jax.ShapeDtypeStruct((4,) + kv.shape, kv.dtype),
        in_specs=[vmem], out_specs=vmem,
        scratch_shapes=[dma((1,)), dma((3,)), dma((3,))],
        name='share_kv' + str(call_id),
        cost_estimate=pl.CostEstimate(flops=20 * 15_000_000, bytes_accessed=1 << 22, transcendentals=0),
        compiler_params=pltpu.CompilerParams(collective_id=call_id, has_side_effects=True),
    )(kv)


def head_norm(values, scale_row):
    mean_sq = jnp.mean(values * values, axis=-1, keepdims=True)
    return values * lax.rsqrt(mean_sq + NORM_EPS) * (1.0 + scale_row)


def rope_tables(positions, head_dim, rope_base, pos_factor):
    exponents = jnp.arange(0, head_dim, 2).astype(jnp.float32) / head_dim
    inv_freq = rope_base ** (-exponents)
    angles = (positions.astype(jnp.float32) / pos_factor)[:, None] * inv_freq[None, :]
    return jnp.cos(angles), jnp.sin(angles)


def apply_rope(values, cos_tab, sin_tab):
    half_dim = values.shape[-1] // 2
    first_half = values[..., :half_dim]
    second_half = values[..., half_dim:]
    cos_bcast = cos_tab[:, None, :]
    sin_bcast = sin_tab[:, None, :]
    return jnp.concatenate([first_half * cos_bcast - second_half * sin_bcast, second_half * cos_bcast + first_half * sin_bcast], axis=-1)


def attend(q, keys, values, seg_q, pos_q, seg_ids, positions, window):
    scores = jnp.einsum('qgd,td->gqt', q, keys, preferred_element_type=jnp.float32) * (q.shape[-1] ** -0.5)
    gap = pos_q[:, None] - positions[None, :]
    allowed = (seg_q[:, None] == seg_ids[None, :]) & (gap >= 0) & (gap < window)
    scores = jnp.where(allowed[None], scores, -1e30)
    exp_scores = jnp.exp(scores - jnp.max(scores, axis=-1, keepdims=True))
    probs = (exp_scores / jnp.sum(exp_scores, axis=-1, keepdims=True)).astype(jnp.bfloat16)
    out = jnp.einsum('gqt,td->qgd', probs, values, preferred_element_type=jnp.float32)
    return out.astype(jnp.bfloat16).reshape(q.shape[0], -1)


def solution(mesh):
    col_spec = P(None, 'model', 'heads')
    row_spec = P(None, 'heads', 'model')
    cache_spec = P(None, None, 'heads', None)
    over_core = [(0, 1), (1, 0), (2, 3), (3, 2)]
    over_x = [(0, 2), (2, 0), (1, 3), (3, 1)]

    def spread(w):
        by_x = lax.ppermute(w, 'model', over_x)
        return [w, lax.ppermute(w, 'model', over_core), by_x, lax.ppermute(by_x, 'model', over_core)]

    def body(hidden_in, seg_ids, positions, w_query, w_key, w_value, w_out, w_gate, w_up, w_down, norm_scales, qk_scales):
        n_tok = hidden_in.shape[0]
        head_dim = qk_scales.shape[-1]
        m = lax.axis_index('model')
        n_own = n_tok // 4
        scales = jnp.stack(spread(norm_scales))[:, :, :, None, :]
        seg_q = lax.dynamic_slice_in_dim(seg_ids, m * n_own, n_own)
        pos_q = lax.dynamic_slice_in_dim(positions, m * n_own, n_own)

        def dot(a, b):
            return jnp.dot(a, b, preferred_element_type=jnp.float32)

        def summed(g, ws):
            acc = dot(g[0], ws[0])
            for j in (1, 2, 3):
                acc = acc + dot(g[j], ws[j])
            return acc.astype(jnp.bfloat16)

        def chunks(a, ws):
            return jnp.stack([dot(a, w) for w in ws]).reshape(4, 4, 2, N_ROWS, 960)

        rows, gathered = move('first', 0, hidden_in.reshape(4, 8, N_ROWS, 960), scales[:, 0, 0])
        settings = ((GLOBAL_BASE, GLOBAL_FACTOR, n_tok), (LOCAL_BASE, 1.0, WINDOW))
        key_list, value_list = [], []
        for l in range(2):
            rope_base, pos_factor, window = settings[l]
            wq, wk, wv, wo, wg, wu, wd = [spread(w[l]) for w in (w_query, w_key, w_value, w_out, w_gate, w_up, w_down)]
            g = gathered.reshape(4, n_own, 960)
            cos_tab, sin_tab = rope_tables(pos_q, head_dim, rope_base, pos_factor)

            def heads_of(ws, row):
                vals = summed(g, ws).astype(jnp.float32).reshape(n_own, -1, head_dim)
                return apply_rope(head_norm(vals, qk_scales[l, row]), cos_tab, sin_tab).astype(jnp.bfloat16)

            q = heads_of(wq, 0)
            k = heads_of(wk, 1)
            v = summed(g, wv)
            kv = share_kv(1 + 4 * l, jnp.stack([k.reshape(n_own, head_dim), v]))
            keys = kv[:, 0].reshape(n_tok, head_dim)
            values = kv[:, 1].reshape(n_tok, head_dim)
            key_list.append(keys)
            value_list.append(values)
            o = attend(q, keys, values, seg_q, pos_q, seg_ids, positions, window)
            rows, gathered = move('mid', 2 + 4 * l, chunks(o, wo), rows, scales[:, l, 1], scales[:, l, 2])
            g = gathered.reshape(4, n_own, 960)
            gate = jax.nn.gelu(summed(g, wg).astype(jnp.float32), approximate=True)
            mid = (gate * summed(g, wu).astype(jnp.float32)).astype(jnp.bfloat16)
            part = chunks(mid, wd)
            if l == 0:
                rows, gathered = move('mid', 3 + 4 * l, part, rows, scales[:, l, 3], scales[:, 1, 0])
            else:
                hidden, = move('last', 3 + 4 * l, part, rows, scales[:, l, 3])
        return hidden.reshape(n_tok, 960), jnp.stack(key_list)[:, :, None], jnp.stack(value_list)[:, :, None]

    return jax.shard_map(body, mesh=mesh,
                         in_specs=(P(None, 'model'), P(), P(), col_spec, col_spec, col_spec, row_spec, col_spec, col_spec, row_spec, P(None, None, 'model'), P()),
                         out_specs=(P(None, 'model'), cache_spec, cache_spec),
                         check_vma=False)
```
